32 devices in a mesh: ent: 2 (over x), blk: 4 (over y, core), rel: 4 (over z).
Axes of the slice: x: 2, y: 2, z: 4, core: 2. Of those that a mesh axis runs over, the one named last changes fastest.
Arguments:
- factors: bfloat16 [8192, 256], P(('ent', 'blk')), may hold values from -12 to 12
- heads: int32 [8, 4, 1, 8192], P(None, 'rel', None, ('ent', 'blk')), may hold values from 0 to 1023, as said below
- tails: int32 [8, 4, 1, 8192], P(None, 'rel', None, ('ent', 'blk')), may hold values from 0 to 1023, as said below
- values: float32 [8, 4, 1, 8192], P(None, 'rel', None, ('ent', 'blk')), may hold values from 0.3 to 9
Outputs:
- relation_fit: float32 [32, 256, 256], P(('ent', 'blk', 'rel'))
- residual: float32 [32, 256, 256], P(('ent', 'blk', 'rel'))
The draws below stay inside these ranges and needn't reach their ends.
Inputs may be any that keep to these rules, and one draw needn't show every extreme that they name: In every aligned tile of 128 triple columns (columns 128 t to 128 t + 127 of one relation) all heads lie in one aligned block of 128 positions (128 b to 128 b + 127). In every aligned tile of 128 triple columns all tails lie in one aligned block of 128 positions.
All inputs are finite; a program needn't handle non-finite values.
Results may differ from the reference program's by a relative error of at most 0.0029.
Values sent between devices are 32-bit elements; how exact they have to be, the bound alone decides.
A program may use at most 128 MiB of HBM per device.

```python
import math
import jax
import jax.numpy as jnp
from jax import lax

RANK = 256
ENT_DEV = 1024
TRIP = 1024
REL_DEV = 1
ITERS = 8
SHARDS = 8
ENTS = 8192
RELS = 32
N_REL = 4


def draw_factors(key, part):
    keys = jax.random.split(jax.random.fold_in(key, 11), 3)
    entries = jnp.clip(jax.random.normal(keys[0], (ENTS, RANK), jnp.float32), -6.0, 6.0)
    columns = jnp.exp(jax.random.uniform(keys[1], (RANK,), jnp.float32, math.log(0.1), 0.0))
    row_scale = jnp.exp(jax.random.uniform(keys[2], (ENTS, 1), jnp.float32, math.log(0.5), math.log(2.0)))
    return (entries * columns[None, :] * row_scale).astype(jnp.bfloat16)


def tiled_positions(key, salt):
    keys = jax.random.split(jax.random.fold_in(key, salt), 2)
    tile_count = SHARDS * TRIP // 128
    block_ids = jax.random.randint(keys[0], (SHARDS, N_REL, REL_DEV, tile_count, 1), 0, ENT_DEV // 128, jnp.int32)
    inside = jax.random.randint(keys[1], (SHARDS, N_REL, REL_DEV, tile_count, 128), 0, 128, jnp.int32)
    return (block_ids * 128 + inside).reshape(SHARDS, N_REL, REL_DEV, SHARDS * TRIP).astype(jnp.int32)


def draw_heads(key, part):
    return tiled_positions(key, 31)


def draw_tails(key, part):
    return tiled_positions(key, 47)


def draw_values(key, part):
    shape_all = (SHARDS, N_REL, REL_DEV, SHARDS * TRIP)
    sub_key = jax.random.fold_in(key, 23)
    base_values = jnp.exp(jax.random.uniform(sub_key, shape_all, jnp.float32, math.log(0.5), math.log(2.0)))
    first_index = jnp.arange(SHARDS, dtype=jnp.int32)[:, None, None, None]
    second_index = jnp.arange(N_REL, dtype=jnp.int32)[None, :, None, None]
    third_index = jnp.arange(REL_DEV, dtype=jnp.int32)[None, None, :, None]
    relation_index = ((first_index * N_REL + second_index) * REL_DEV + third_index).astype(jnp.float32)
    rising = 1.0 + 2.0 * relation_index / max(RELS - 1, 1)
    return (base_values * rising).astype(jnp.float32)


def setup_inputs(seed: int = 0) -> dict:
    streams_of = jax.random.split(jax.random.key(seed), 5)
    factors = draw_factors(jax.random.fold_in(streams_of[4], 71), 0)
    heads = draw_heads(jax.random.fold_in(streams_of[4], 71), 0)
    tails = draw_tails(jax.random.fold_in(streams_of[4], 71), 0)
    values = draw_values(jax.random.fold_in(streams_of[4], 71), 0)
    return dict(factors=factors, heads=heads, tails=tails, values=values)


ridge_weight = 0.01

def apply_normal(gram_matrix, stacked):
    left_side = jnp.einsum('ab,kbc->kac', gram_matrix, stacked, precision=lax.Precision.HIGHEST)
    return jnp.einsum('kac,cd->kad', left_side, gram_matrix, precision=lax.Precision.HIGHEST) + ridge_weight * stacked

def reference(factors, heads, tails, values):
    gram_matrix = jnp.dot(factors.T, factors, preferred_element_type=jnp.float32) / ENTS
    column_ids = jnp.arange(SHARDS * TRIP, dtype=jnp.int32)
    offsets = (column_ids // TRIP * ENT_DEV).astype(jnp.int32)
    head_ids = (heads.reshape(RELS, SHARDS * TRIP) + offsets).astype(jnp.int32)
    tail_ids = (tails.reshape(RELS, SHARDS * TRIP) + offsets).astype(jnp.int32)
    weights = values.reshape(RELS, SHARDS * TRIP)
    norm_scale = 1.0 / math.sqrt(SHARDS * TRIP)

    def single(operands):
        head_row, tail_row, weight_row = operands
        weighted = (weight_row[:, None] * jnp.take(factors, head_row, axis=0).astype(jnp.float32)).astype(jnp.bfloat16)
        tail_rows = jnp.take(factors, tail_row, axis=0)
        return jnp.dot(weighted.T, tail_rows, preferred_element_type=jnp.float32) * norm_scale
    target = lax.map(single, (head_ids, tail_ids, weights))
    fitted = jnp.zeros_like(target)
    residual = target
    direction = target
    norm_now = jnp.sum(residual * residual)
    for step_index in range(ITERS):
        image_map = apply_normal(gram_matrix, direction)
        step_size = norm_now / jnp.sum(direction * image_map)
        fitted = fitted + step_size * direction
        residual = residual - step_size * image_map
        norm_next = jnp.sum(residual * residual)
        direction = residual + norm_next / norm_now * direction
        norm_now = norm_next
    return (fitted, residual)
```

```python
import functools
import math

import jax
import jax.numpy as jnp
from jax import lax
from jax.experimental import pallas as pl
from jax.experimental.pallas import tpu as pltpu
from jax.sharding import PartitionSpec as P

ITERS = 8


ridge_weight = 0.01
tile_width = 128


def apply_normal(gram_matrix, stacked):
    left_side = jnp.einsum("ab,kbc->kac", gram_matrix, stacked, precision=lax.Precision.HIGHEST)
    return (
        jnp.einsum("kac,cd->kad", left_side, gram_matrix, precision=lax.Precision.HIGHEST)
        + ridge_weight * stacked
    )


def two_products(residual, image_map):
    return lax.psum(
        (jnp.sum(residual * residual), jnp.sum(residual * image_map)), ("ent", "blk", "rel")
    )


def select_rows(entity_ids, block_table):
    group_size, width = entity_ids.shape
    tile_count = width // tile_width
    block_count = block_table.shape[0]
    tiled_ids = entity_ids.reshape(group_size, tile_count, tile_width)
    block_of = tiled_ids[:, :, 0] // tile_width
    block_pick = (
        block_of[:, :, None] == jnp.arange(block_count, dtype=jnp.int32)[None, None, :]
    ).astype(jnp.bfloat16)
    chosen = jnp.einsum(
        "gtb,bcr->gtcr", block_pick, block_table, preferred_element_type=jnp.float32
    ).astype(jnp.bfloat16)
    inside = tiled_ids % tile_width
    slot_pick = (
        inside[:, :, :, None] == jnp.arange(tile_width, dtype=jnp.int32)[None, None, None, :]
    ).astype(jnp.bfloat16)
    return jnp.einsum("gtoc,gtcr->gtor", slot_pick, chosen, preferred_element_type=jnp.float32)


def body(factors, heads, tails, values):
    shards = lax.axis_size(("ent", "blk"))
    ent_dev = factors.shape[0]
    rank_width = factors.shape[1]
    triple_count = heads.shape[3]
    relation_rows = heads.shape[0] * heads.shape[2]
    norm_scale = 1.0 / math.sqrt(shards * triple_count)
    gram_total = lax.psum(
        jnp.dot(factors.T, factors, preferred_element_type=jnp.float32), ("ent", "blk")
    )
    gram_matrix = gram_total / (ent_dev * shards)
    block_table = factors.reshape(ent_dev // tile_width, tile_width, rank_width)
    head_ids = heads.reshape(relation_rows, triple_count)
    tail_ids = tails.reshape(relation_rows, triple_count)
    weights = values.reshape(relation_rows, triple_count)

    def grouped(operands):
        head_group, tail_group, weight_group = operands
        group_size = head_group.shape[0]
        tile_count = triple_count // tile_width
        head_rows = select_rows(head_group, block_table)
        weighted = (
            weight_group.reshape(group_size, tile_count, tile_width)[:, :, :, None] * head_rows
        ).astype(jnp.bfloat16)
        tail_rows = select_rows(tail_group, block_table).astype(jnp.bfloat16)
        product = jnp.einsum(
            "gtci,gtcj->gij", weighted, tail_rows, preferred_element_type=jnp.float32
        )
        return product * norm_scale

    own_rows = relation_rows // shards
    group_size = math.gcd(own_rows * lax.axis_size(("ent", "blk")), 4)
    group_total = own_rows * lax.axis_size(("ent", "blk")) // group_size
    shaped = (
        head_ids.reshape(group_total, group_size, triple_count),
        tail_ids.reshape(group_total, group_size, triple_count),
        weights.reshape(group_total, group_size, triple_count),
    )
    results = lax.map(grouped, shaped)
    target = lax.psum_scatter(
        results.reshape(own_rows * lax.axis_size(("ent", "blk")), rank_width, rank_width),
        ("ent", "blk"),
        scatter_dimension=0,
        tiled=True,
    )
    fitted = jnp.zeros_like(target)
    residual = target
    image_map = apply_normal(gram_matrix, residual)
    norm_now, product = two_products(residual, image_map)
    step_size = norm_now / product
    direction = residual
    along = image_map
    for step_index in range(ITERS):
        fitted = fitted + step_size * direction
        residual = residual - step_size * along
        if step_index + 1 < ITERS:
            image_map = apply_normal(gram_matrix, residual)
            norm_next, product = two_products(residual, image_map)
            ratio_next = norm_next / norm_now
            step_size = norm_next / (product - ratio_next * norm_next / step_size)
            direction = residual + ratio_next * direction
            along = image_map + ratio_next * along
            norm_now = norm_next
    return (fitted, residual)


MESH = pl.DeviceIdType.MESH
COPIES = 32


def fused_kernel(
    z_count, scale_gram, scale_target,
    factors_ref, heads_ref, tails_ref, values_ref, head_ids, tail_ids,
    fit_ref, res_ref,
    turned, left_rows, right_rows,
    gram_part, gram_in, gram_half, gram_xy, gram_full, gram_pair,
    pair_out, pair_in, own_sum, first_a, first_b, second_a, second_b,
    basis, table, send_sem, recv_sem,
):
    f32, bf16 = jnp.float32, jnp.bfloat16
    width = factors_ref.shape[1]
    half = width // 2
    quarter = width // 4
    triples = heads_ref.shape[3]
    e = lax.axis_index("ent")
    b = lax.axis_index("blk")
    z = lax.axis_index("rel")
    y = b // 2
    c = b % 2
    pair_peer = (e, y * 2 + 1 - c, z)
    x_peer = (1 - e, b, z)
    y_peer = (e, (1 - y) * 2 + c, z)

    def group_peer(mask):
        me, my, mc = mask // 4, (mask // 2) % 2, mask % 2
        return (
            (1 - e) if me else e,
            ((1 - y) if my else y) * 2 + ((1 - c) if mc else c),
            z,
        )

    def z_peer(hop):
        return (e, b, lax.rem(z + hop, z_count))

    peers = [group_peer(m) for m in range(1, 8)] + [z_peer(h) for h in range(1, z_count)]
    barrier = pltpu.get_barrier_semaphore()
    for peer in peers:
        pl.semaphore_signal(barrier, inc=1, device_id=peer, device_id_type=MESH)

    counter = [0]

    def send(source, dest, peer):
        slot = counter[0]
        counter[0] += 1
        copy = pltpu.make_async_remote_copy(
            src_ref=source, dst_ref=dest,
            send_sem=send_sem.at[slot], recv_sem=recv_sem.at[slot],
            device_id=peer, device_id_type=MESH,
        )
        copy.start()
        return copy

    flipped = factors_ref[...].T
    for block in range(turned.shape[0]):
        turned[block] = flipped[:, block * tile_width : (block + 1) * tile_width]
    gram_part[...] = lax.dot_general(
        flipped, flipped, (((1,), (1,)), ((), ())), preferred_element_type=f32
    )
    pl.semaphore_wait(barrier, len(peers))
    own_rows = pl.ds(pl.multiple_of(c * half, half), half)
    other_rows = pl.ds(pl.multiple_of((1 - c) * half, half), half)
    g_pair = send(gram_part.at[other_rows], gram_in, pair_peer)

    row_number = lax.broadcasted_iota(jnp.int32, (tile_width, tile_width), 0)
    blank = jnp.zeros((tile_width, tile_width), bf16)

    def gathered(ids_ref, scalar_ref, q, first):
        picks, blocks = [], []
        for tile in (first, first + 1):
            start = tile * tile_width
            inside = lax.rem(ids_ref[q, 0, :, start : start + tile_width], tile_width)
            picks.append(jnp.where(row_number == inside, 1.0, 0.0).astype(bf16))
            blocks.append(turned[lax.div(scalar_ref[q, 0, 0, start], tile_width)])
        mixed = jnp.concatenate(
            [
                jnp.concatenate([picks[0], blank], axis=1),
                jnp.concatenate([blank, picks[1]], axis=1),
            ],
            axis=0,
        )
        return jnp.dot(jnp.concatenate(blocks, axis=1), mixed, preferred_element_type=f32)

    def partial(pe, py, pc):
        q = pe * 4 + py * 2 + pc
        for first in range(0, triples // tile_width, 2):
            cols = slice(first * tile_width, (first + 2) * tile_width)
            rows = gathered(heads_ref, head_ids, q, first)
            left_rows[:, cols] = (values_ref[q, 0, :, cols] * rows).astype(bf16)
            right_rows[:, cols] = gathered(tails_ref, tail_ids, q, first).astype(bf16)
        return lax.dot_general(
            left_rows[...], right_rows[...], (((1,), (1,)), ((), ())), preferred_element_type=f32
        )

    targets = ((1 - e, 1 - y), (1 - e, y), (e, 1 - y), (e, y))
    pair_copies = []

    def give(index):
        pe, py = targets[index]
        pair_out[index] = partial(pe, py, 1 - c)
        pair_copies.append(send(pair_out.at[index], pair_in.at[index], pair_peer))

    def keep(index):
        pe, py = targets[index]
        own_sum[index] = partial(pe, py, c)
        pair_copies[index].wait()
        own_sum[index] = own_sum[index] + pair_in[index]

    top, low = pl.ds(0, half), pl.ds(half, half)
    give(0)
    g_pair.wait()
    gram_half[0] = gram_part[own_rows, :] + gram_in[...]
    g_a1 = send(gram_half.at[0, pl.ds(0, quarter)], gram_xy.at[0, pl.ds(0, quarter)], x_peer)
    g_b1 = send(
        gram_half.at[0, pl.ds(quarter, quarter)], gram_xy.at[0, pl.ds(quarter, quarter)], y_peer
    )
    keep(0)
    a_diag = send(own_sum.at[0, top], first_a.at[0], x_peer)
    b_diag = send(own_sum.at[0, low], first_b.at[0], y_peer)
    give(1)
    g_a1.wait()
    g_b1.wait()
    gram_half[1] = gram_half[0] + gram_xy[0]
    g_a2 = send(gram_half.at[1, pl.ds(0, quarter)], gram_xy.at[1, pl.ds(0, quarter)], y_peer)
    g_b2 = send(
        gram_half.at[1, pl.ds(quarter, quarter)], gram_xy.at[1, pl.ds(quarter, quarter)], x_peer
    )
    keep(1)
    a_side = send(own_sum.at[1, top], first_a.at[1], x_peer)
    give(2)
    keep(2)
    b_side = send(own_sum.at[2, low], first_b.at[1], y_peer)
    a_diag.wait()
    second_a[0] = own_sum[2, :half, :] + first_a[0]
    a_last = send(second_a.at[0], second_a.at[1], y_peer)
    b_diag.wait()
    second_b[0] = own_sum[1, half:, :] + first_b[0]
    b_last = send(second_b.at[0], second_b.at[1], x_peer)
    g_a2.wait()
    g_b2.wait()
    gram_pair[0] = gram_half[1] + gram_xy[1]
    g_full = send(gram_pair.at[0], gram_pair.at[1], pair_peer)
    give(3)
    keep(3)
    g_full.wait()
    gram_full[own_rows, :] = gram_pair[0] * scale_gram
    gram_full[other_rows, :] = gram_pair[1] * scale_gram
    gram = gram_full[...]
    gram_high = gram.astype(bf16)
    gram_low = (gram - gram_high.astype(f32)).astype(bf16)
    gram_both = jnp.concatenate([gram_high, gram_low], axis=0)
    a_side.wait()
    b_side.wait()
    a_last.wait()
    b_last.wait()
    basis[0, :half, :] = ((own_sum[3, :half, :] + first_a[1]) + second_a[1]) * scale_target
    basis[0, half:, :] = ((own_sum[3, half:, :] + first_b[1]) + second_b[1]) * scale_target

    def split(value):
        high = value.astype(bf16)
        return high, (value - high.astype(f32)).astype(bf16)

    def total(value):
        return jnp.sum(jnp.sum(value, axis=0, keepdims=True), axis=1, keepdims=True)

    def normal_map(value):
        high, low_part = split(value)
        both = jnp.dot(gram_both, high, preferred_element_type=f32)
        inner = both[:width] + (
            both[width:] + jnp.dot(gram_high, low_part, preferred_element_type=f32)
        )
        high, low_part = split(inner)
        both = jnp.dot(
            jnp.concatenate([high, low_part], axis=0), gram_high, preferred_element_type=f32
        )
        outer = both[:width] + (
            both[width:] + jnp.dot(high, gram_low, preferred_element_type=f32)
        )
        return outer + ridge_weight * value

    lane = lax.broadcasted_iota(jnp.int32, (1, 128), 1)
    record = jnp.zeros((1, 128), f32)
    inverses = []
    for index in range(ITERS):
        vector = basis[index]
        image = normal_map(vector)
        square = total(vector * vector)
        cross = total(vector * image)
        inverse = jnp.where(square > 0.0, lax.rsqrt(square), 0.0)
        length = square * inverse
        diagonal = (cross * inverse) * inverse
        record = jnp.where(lane == index, diagonal, record)
        record = jnp.where(lane == ITERS + index, length, record)
        if index + 1 == ITERS:
            table[0, 0] = record
            z_copies = [
                send(table.at[0, 0], table.at[0, z_count - hop], z_peer(hop))
                for hop in range(1, z_count)
            ]
        following = (image - diagonal * vector) * inverse
        if index > 0:
            following = following - (length * inverses[-1]) * basis[index - 1]
        inverses.append(inverse)
        basis[index + 1] = following
    for copy in z_copies:
        copy.wait()
    group_copies = [send(table.at[0], table.at[m], group_peer(m)) for m in range(1, 8)]
    for copy in group_copies:
        copy.wait()

    lines = table[...].reshape(8 * z_count, 128)
    filled = jnp.concatenate([lines, jnp.zeros((128 - 8 * z_count, 128), f32)], axis=0).T
    alpha = [filled[j : j + 1, :] for j in range(ITERS)]
    beta = [filled[ITERS + j : ITERS + j + 1, :] for j in range(ITERS)] + [
        jnp.ones((1, 128), f32)
    ]

    def reduced(rows):
        added = rows[0]
        for row in rows[1:]:
            added = added + row
        return jnp.sum(added, axis=1, keepdims=True)

    def small_map(rows):
        count = len(rows)
        made = []
        for j in range(count + 1):
            entry = None
            if j < count:
                entry = alpha[j] * rows[j]
            if j > 0:
                term = beta[j] * rows[j - 1]
                entry = term if entry is None else entry + term
            if j + 1 < count:
                entry = entry + beta[j + 1] * rows[j + 1]
            made.append(entry)
        return made

    def mixed_sum(first, ratio, second):
        return [
            one + ratio * second[j] if j < len(second) else one for j, one in enumerate(first)
        ]

    residual = [beta[0]]
    image = small_map(residual)
    norm_now = reduced([row * row for row in residual])
    product = reduced([row * image[j] for j, row in enumerate(residual)])
    step_size = norm_now / product
    direction, along = residual, image
    fitted = []
    for index in range(ITERS):
        fitted = [
            fitted[j] + step_size * row if j < len(fitted) else step_size * row
            for j, row in enumerate(direction)
        ]
        residual = [
            residual[j] - step_size * row if j < len(residual) else -(step_size * row)
            for j, row in enumerate(along)
        ]
        if index + 1 < ITERS:
            image = small_map(residual)
            norm_next = reduced([row * row for row in residual])
            product = reduced([row * image[j] for j, row in enumerate(residual)])
            ratio = norm_next / norm_now
            step_size = norm_next / (product - ratio * norm_next / step_size)
            direction = mixed_sum(residual, ratio, direction)
            along = mixed_sum(image, ratio, along)
            norm_now = norm_next
    inverses.append(jnp.ones((1, 1), f32))
    fit_weights = [row[:, 0:1] * inverses[j] for j, row in enumerate(fitted)]
    res_weights = [row[:, 0:1] * inverses[j] for j, row in enumerate(residual)]
    fit = fit_weights[0] * basis[0]
    res = res_weights[0] * basis[0]
    for j in range(1, ITERS):
        fit = fit + fit_weights[j] * basis[j]
        res = res + res_weights[j] * basis[j]
    fit_ref[0] = fit
    res_ref[0] = res + res_weights[ITERS] * basis[ITERS]


def fused_body(factors, heads, tails, values):
    shards = lax.axis_size(("ent", "blk"))
    z_count = lax.axis_size("rel")
    ent_dev, width = factors.shape
    triples = heads.shape[3]
    half = width // 2
    f32, bf16 = jnp.float32, jnp.bfloat16
    vmem = pl.BlockSpec(memory_space=pltpu.VMEM)
    smem = pl.BlockSpec(memory_space=pltpu.SMEM)
    out = jax.ShapeDtypeStruct((1, width, width), f32)
    return pl.pallas_call(
        functools.partial(
            fused_kernel, z_count, 1.0 / (ent_dev * shards), 1.0 / math.sqrt(shards * triples)
        ),
        out_shape=(out, out),
        in_specs=[vmem] * 4 + [smem] * 2,
        out_specs=(vmem, vmem),
        scratch_shapes=[
            pltpu.VMEM((ent_dev // tile_width, width, tile_width), bf16),
            pltpu.VMEM((width, triples), bf16),
            pltpu.VMEM((width, triples), bf16),
            pltpu.VMEM((width, width), f32),
            pltpu.VMEM((half, width), f32),
            pltpu.VMEM((2, half, width), f32),
            pltpu.VMEM((2, half, width), f32),
            pltpu.VMEM((width, width), f32),
            pltpu.VMEM((2, half, width), f32),
            pltpu.VMEM((4, width, width), f32),
            pltpu.VMEM((4, width, width), f32),
            pltpu.VMEM((4, width, width), f32),
            pltpu.VMEM((2, half, width), f32),
            pltpu.VMEM((2, half, width), f32),
            pltpu.VMEM((2, half, width), f32),
            pltpu.VMEM((2, half, width), f32),
            pltpu.VMEM((ITERS + 1, width, width), f32),
            pltpu.VMEM((8, z_count, 1, 128), f32),
            pltpu.SemaphoreType.DMA((COPIES,)),
            pltpu.SemaphoreType.DMA((COPIES,)),
        ],
        compiler_params=pltpu.CompilerParams(collective_id=0, has_side_effects=True),
    )(factors, heads, tails, values, heads, tails)


def solution(mesh):
    placed = (
        P(("ent", "blk"), None),
        P(None, "rel", None, ("ent", "blk")),
        P(None, "rel", None, ("ent", "blk")),
        P(None, "rel", None, ("ent", "blk")),
    )
    sizes = dict(mesh.shape)
    fused = sizes["ent"] == 2 and sizes["blk"] == 4 and 1 < sizes["rel"] <= 16
    return jax.shard_map(
        fused_body if fused else body,
        mesh=mesh,
        in_specs=placed,
        out_specs=(P(("ent", "blk", "rel"), None, None), P(("ent", "blk", "rel"), None, None)),
        check_vma=False,
    )
```

```python
import functools
import math

import jax
import jax.numpy as jnp
from jax import lax
from jax.experimental import pallas as pl
from jax.experimental.pallas import tpu as pltpu
from jax.sharding import PartitionSpec as P

ITERS = 8


ridge_weight = 0.01
tile_width = 128


def apply_normal(gram_matrix, stacked):
    left_side = jnp.einsum("ab,kbc->kac", gram_matrix, stacked, precision=lax.Precision.HIGHEST)
    return (
        jnp.einsum("kac,cd->kad", left_side, gram_matrix, precision=lax.Precision.HIGHEST)
        + ridge_weight * stacked
    )


def two_products(residual, image_map):
    return lax.psum(
        (jnp.sum(residual * residual), jnp.sum(residual * image_map)), ("ent", "blk", "rel")
    )


def select_rows(entity_ids, block_table):
    group_size, width = entity_ids.shape
    tile_count = width // tile_width
    block_count = block_table.shape[0]
    tiled_ids = entity_ids.reshape(group_size, tile_count, tile_width)
    block_of = tiled_ids[:, :, 0] // tile_width
    block_pick = (
        block_of[:, :, None] == jnp.arange(block_count, dtype=jnp.int32)[None, None, :]
    ).astype(jnp.bfloat16)
    chosen = jnp.einsum(
        "gtb,bcr->gtcr", block_pick, block_table, preferred_element_type=jnp.float32
    ).astype(jnp.bfloat16)
    inside = tiled_ids % tile_width
    slot_pick = (
        inside[:, :, :, None] == jnp.arange(tile_width, dtype=jnp.int32)[None, None, None, :]
    ).astype(jnp.bfloat16)
    return jnp.einsum("gtoc,gtcr->gtor", slot_pick, chosen, preferred_element_type=jnp.float32)


def body(factors, heads, tails, values):
    shards = lax.axis_size(("ent", "blk"))
    ent_dev = factors.shape[0]
    rank_width = factors.shape[1]
    triple_count = heads.shape[3]
    relation_rows = heads.shape[0] * heads.shape[2]
    norm_scale = 1.0 / math.sqrt(shards * triple_count)
    gram_total = lax.psum(
        jnp.dot(factors.T, factors, preferred_element_type=jnp.float32), ("ent", "blk")
    )
    gram_matrix = gram_total / (ent_dev * shards)
    block_table = factors.reshape(ent_dev // tile_width, tile_width, rank_width)
    head_ids = heads.reshape(relation_rows, triple_count)
    tail_ids = tails.reshape(relation_rows, triple_count)
    weights = values.reshape(relation_rows, triple_count)

    def grouped(operands):
        head_group, tail_group, weight_group = operands
        group_size = head_group.shape[0]
        tile_count = triple_count // tile_width
        head_rows = select_rows(head_group, block_table)
        weighted = (
            weight_group.reshape(group_size, tile_count, tile_width)[:, :, :, None] * head_rows
        ).astype(jnp.bfloat16)
        tail_rows = select_rows(tail_group, block_table).astype(jnp.bfloat16)
        product = jnp.einsum(
            "gtci,gtcj->gij", weighted, tail_rows, preferred_element_type=jnp.float32
        )
        return product * norm_scale

    own_rows = relation_rows // shards
    group_size = math.gcd(own_rows * lax.axis_size(("ent", "blk")), 4)
    group_total = own_rows * lax.axis_size(("ent", "blk")) // group_size
    shaped = (
        head_ids.reshape(group_total, group_size, triple_count),
        tail_ids.reshape(group_total, group_size, triple_count),
        weights.reshape(group_total, group_size, triple_count),
    )
    results = lax.map(grouped, shaped)
    target = lax.psum_scatter(
        results.reshape(own_rows * lax.axis_size(("ent", "blk")), rank_width, rank_width),
        ("ent", "blk"),
        scatter_dimension=0,
        tiled=True,
    )
    fitted = jnp.zeros_like(target)
    residual = target
    image_map = apply_normal(gram_matrix, residual)
    norm_now, product = two_products(residual, image_map)
    step_size = norm_now / product
    direction = residual
    along = image_map
    for step_index in range(ITERS):
        fitted = fitted + step_size * direction
        residual = residual - step_size * along
        if step_index + 1 < ITERS:
            image_map = apply_normal(gram_matrix, residual)
            norm_next, product = two_products(residual, image_map)
            ratio_next = norm_next / norm_now
            step_size = norm_next / (product - ratio_next * norm_next / step_size)
            direction = residual + ratio_next * direction
            along = image_map + ratio_next * along
            norm_now = norm_next
    return (fitted, residual)


MESH = pl.DeviceIdType.MESH
COPIES = 32


def fused_kernel(
    z_count, scale_gram, scale_target,
    factors_hbm, heads_hbm, tails_hbm, values_hbm,
    fit_ref, res_ref,
    factors_ref, heads_ref, tails_ref, values_ref, head_ids, tail_ids, load_sem, ready,
    turned, left_rows, right_rows,
    gram_part, gram_in, gram_half, gram_xy, gram_line, gram_full, gram_pair,
    pair_out, pair_in, own_sum, first_a, first_b, second_a, second_b,
    basis, table, send_sem, recv_sem,
):
    f32, bf16 = jnp.float32, jnp.bfloat16
    width = factors_ref.shape[1]
    half = width // 2
    share = half // z_count
    part = share // 2
    triples = heads_ref.shape[3]
    e = lax.axis_index("ent")
    b = lax.axis_index("blk")
    z = lax.axis_index("rel")
    y = b // 2
    c = b % 2
    pair_peer = (e, y * 2 + 1 - c, z)
    x_peer = (1 - e, b, z)
    y_peer = (e, (1 - y) * 2 + c, z)

    def group_peer(mask):
        me, my, mc = mask // 4, (mask // 2) % 2, mask % 2
        return (
            (1 - e) if me else e,
            ((1 - y) if my else y) * 2 + ((1 - c) if mc else c),
            z,
        )

    def z_peer(hop):
        return (e, b, lax.rem(z + hop, z_count))

    near = [group_peer(m) for m in (1, 2, 4)]
    inner = ((z > 0, -1), (z < z_count - 1, 1))

    def tell(semaphore):
        for present, hop in inner:
            @pl.when(present)
            def _():
                pl.semaphore_signal(
                    semaphore, inc=1, device_id=(e, b, z + hop), device_id_type=MESH
                )

    line_count = jnp.where(z > 0, 1, 0) + jnp.where(z < z_count - 1, 1, 0)
    barrier = pltpu.get_barrier_semaphore()
    for peer in near:
        pl.semaphore_signal(barrier, inc=1, device_id=peer, device_id_type=MESH)
    tell(barrier)
    loads = []
    for slot, (source, dest) in enumerate(
        (
            (factors_hbm, factors_ref),
            (heads_hbm, head_ids),
            (tails_hbm, tail_ids),
            (heads_hbm, heads_ref),
            (values_hbm, values_ref),
            (tails_hbm, tails_ref),
        )
    ):
        loads.append(pltpu.make_async_copy(source, dest, load_sem.at[slot]))
        loads[-1].start()

    counter = [0]

    def send(source, dest, peer):
        slot = counter[0]
        counter[0] += 1
        copy = pltpu.make_async_remote_copy(
            src_ref=source, dst_ref=dest,
            send_sem=send_sem.at[slot], recv_sem=recv_sem.at[slot],
            device_id=peer, device_id_type=MESH,
        )
        copy.start()
        return copy

    loads[0].wait()
    flipped = factors_ref[...].T
    for block in range(turned.shape[0]):
        turned[block] = flipped[:, block * tile_width : (block + 1) * tile_width]
    gram_part[...] = lax.dot_general(
        flipped, flipped, (((1,), (1,)), ((), ())), preferred_element_type=f32
    )
    own_rows = pl.ds(pl.multiple_of(c * half, half), half)
    other_rows = pl.ds(pl.multiple_of((1 - c) * half, half), half)
    own_share = pl.ds(pl.multiple_of(c * half + z * share, share), share)
    other_share = pl.ds(pl.multiple_of((1 - c) * half + z * share, share), share)

    row_number = lax.broadcasted_iota(jnp.int32, (tile_width, tile_width), 0)
    blank = jnp.zeros((tile_width, tile_width), bf16)

    def gathered(ids_ref, scalar_ref, q, first):
        picks, blocks = [], []
        for tile in (first, first + 1):
            start = tile * tile_width
            inside = lax.rem(ids_ref[q, 0, :, start : start + tile_width], tile_width)
            picks.append(jnp.where(row_number == inside, 1.0, 0.0).astype(bf16))
            blocks.append(turned[lax.div(scalar_ref[q, 0, 0, start], tile_width)])
        mixed = jnp.concatenate(
            [
                jnp.concatenate([picks[0], blank], axis=1),
                jnp.concatenate([blank, picks[1]], axis=1),
            ],
            axis=0,
        )
        return jnp.dot(jnp.concatenate(blocks, axis=1), mixed, preferred_element_type=f32)

    def partial(pe, py, pc):
        q = pe * 4 + py * 2 + pc
        for first in range(0, triples // tile_width, 2):
            cols = slice(first * tile_width, (first + 2) * tile_width)
            rows = gathered(heads_ref, head_ids, q, first)
            left_rows[:, cols] = (values_ref[q, 0, :, cols] * rows).astype(bf16)
            right_rows[:, cols] = gathered(tails_ref, tail_ids, q, first).astype(bf16)
        return lax.dot_general(
            left_rows[...], right_rows[...], (((1,), (1,)), ((), ())), preferred_element_type=f32
        )

    targets = ((1 - e, 1 - y), (1 - e, y), (e, 1 - y), (e, y))
    pair_copies = []

    def give(index):
        pe, py = targets[index]
        pair_out[index] = partial(pe, py, 1 - c)
        pair_copies.append(send(pair_out.at[index], pair_in.at[index], pair_peer))

    def keep(index):
        pe, py = targets[index]
        own_sum[index] = partial(pe, py, c)
        pair_copies[index].wait()
        own_sum[index] = own_sum[index] + pair_in[index]

    top, low = pl.ds(0, half), pl.ds(half, half)
    for load in loads[1:]:
        load.wait()
    pair_out[0] = partial(1 - e, 1 - y, 1 - c)
    pl.semaphore_wait(barrier, len(near) + line_count)
    g_pair = send(gram_part.at[other_share], gram_in, pair_peer)
    pair_copies.append(send(pair_out.at[0], pair_in.at[0], pair_peer))
    for step in range(z_count - 2):
        tell(ready.at[step])
        if step + 1 < z_count - 2:
            pl.semaphore_wait(ready.at[step], line_count)
    g_pair.wait()
    gram_half[0] = gram_part[own_share, :] + gram_in[...]
    upper, lower = pl.ds(0, part), pl.ds(part, part)
    g_a1 = send(gram_half.at[0, upper], gram_xy.at[0, upper], x_peer)
    g_b1 = send(gram_half.at[0, lower], gram_xy.at[0, lower], y_peer)
    keep(0)
    a_diag = send(own_sum.at[0, top], first_a.at[0], x_peer)
    b_diag = send(own_sum.at[0, low], first_b.at[0], y_peer)
    give(1)
    g_a1.wait()
    g_b1.wait()
    gram_half[1] = gram_half[0] + gram_xy[0]
    g_a2 = send(gram_half.at[1, upper], gram_xy.at[1, upper], y_peer)
    g_b2 = send(gram_half.at[1, lower], gram_xy.at[1, lower], x_peer)
    keep(1)
    a_side = send(own_sum.at[1, top], first_a.at[1], x_peer)
    give(2)
    g_a2.wait()
    g_b2.wait()
    gram_line[0] = gram_half[1] + gram_xy[1]
    if z_count > 2:
        pl.semaphore_wait(ready.at[z_count - 3], line_count)
    line_copies = [
        send(gram_line.at[0], gram_line.at[z_count - hop], z_peer(hop))
        for hop in range(1, z_count)
    ]
    keep(2)
    b_side = send(own_sum.at[2, low], first_b.at[1], y_peer)
    a_diag.wait()
    second_a[0] = own_sum[2, :half, :] + first_a[0]
    a_last = send(second_a.at[0], second_a.at[1], y_peer)
    b_diag.wait()
    second_b[0] = own_sum[1, half:, :] + first_b[0]
    b_last = send(second_b.at[0], second_b.at[1], x_peer)
    for copy in line_copies:
        copy.wait()
    for hop in range(z_count):
        place = lax.rem(z + hop, z_count)
        gram_pair[0, pl.ds(pl.multiple_of(place * share, share), share), :] = gram_line[hop]
    g_full = send(gram_pair.at[0], gram_pair.at[1], pair_peer)
    give(3)
    keep(3)
    g_full.wait()
    gram_full[own_rows, :] = gram_pair[0] * scale_gram
    gram_full[other_rows, :] = gram_pair[1] * scale_gram
    gram = gram_full[...]
    gram_high = gram.astype(bf16)
    gram_low = (gram - gram_high.astype(f32)).astype(bf16)
    gram_both = jnp.concatenate([gram_high, gram_low], axis=0)
    a_side.wait()
    b_side.wait()
    a_last.wait()
    b_last.wait()
    basis[0, :half, :] = ((own_sum[3, :half, :] + first_a[1]) + second_a[1]) * scale_target
    basis[0, half:, :] = ((own_sum[3, half:, :] + first_b[1]) + second_b[1]) * scale_target

    def split(value):
        high = value.astype(bf16)
        return high, (value - high.astype(f32)).astype(bf16)

    def total(value):
        return jnp.sum(jnp.sum(value, axis=0, keepdims=True), axis=1, keepdims=True)

    def normal_map(value):
        high, low_part = split(value)
        both = jnp.dot(gram_both, high, preferred_element_type=f32)
        inner = both[:width] + (
            both[width:] + jnp.dot(gram_high, low_part, preferred_element_type=f32)
        )
        high, low_part = split(inner)
        both = jnp.dot(
            jnp.concatenate([high, low_part], axis=0), gram_high, preferred_element_type=f32
        )
        outer = both[:width] + (
            both[width:] + jnp.dot(high, gram_low, preferred_element_type=f32)
        )
        return outer + ridge_weight * value

    lane = lax.broadcasted_iota(jnp.int32, (1, 128), 1)
    record = jnp.zeros((1, 128), f32)
    inverses = []
    for index in range(ITERS):
        vector = basis[index]
        image = normal_map(vector)
        square = total(vector * vector)
        cross = total(vector * image)
        inverse = jnp.where(square > 0.0, lax.rsqrt(square), 0.0)
        length = square * inverse
        diagonal = (cross * inverse) * inverse
        record = jnp.where(lane == index, diagonal, record)
        record = jnp.where(lane == ITERS + index, length, record)
        if index + 1 == ITERS:
            table[0, 0] = record
            z_copies = [
                send(table.at[0, 0], table.at[0, z_count - hop], z_peer(hop))
                for hop in range(1, z_count)
            ]
        following = (image - diagonal * vector) * inverse
        if index > 0:
            following = following - (length * inverses[-1]) * basis[index - 1]
        inverses.append(inverse)
        basis[index + 1] = following
    for copy in z_copies:
        copy.wait()
    group_copies = [send(table.at[0], table.at[m], group_peer(m)) for m in range(1, 8)]
    for copy in group_copies:
        copy.wait()

    lines = table[...].reshape(8 * z_count, 128)
    filled = jnp.concatenate([lines, jnp.zeros((128 - 8 * z_count, 128), f32)], axis=0).T
    alpha = [filled[j : j + 1, :] for j in range(ITERS)]
    beta = [filled[ITERS + j : ITERS + j + 1, :] for j in range(ITERS)] + [
        jnp.ones((1, 128), f32)
    ]

    def reduced(rows):
        added = rows[0]
        for row in rows[1:]:
            added = added + row
        return jnp.sum(added, axis=1, keepdims=True)

    def small_map(rows):
        count = len(rows)
        made = []
        for j in range(count + 1):
            entry = None
            if j < count:
                entry = alpha[j] * rows[j]
            if j > 0:
                term = beta[j] * rows[j - 1]
                entry = term if entry is None else entry + term
            if j + 1 < count:
                entry = entry + beta[j + 1] * rows[j + 1]
            made.append(entry)
        return made

    def mixed_sum(first, ratio, second):
        return [
            one + ratio * second[j] if j < len(second) else one for j, one in enumerate(first)
        ]

    residual = [beta[0]]
    image = small_map(residual)
    norm_now = reduced([row * row for row in residual])
    product = reduced([row * image[j] for j, row in enumerate(residual)])
    step_size = norm_now / product
    direction, along = residual, image
    fitted = []
    for index in range(ITERS):
        fitted = [
            fitted[j] + step_size * row if j < len(fitted) else step_size * row
            for j, row in enumerate(direction)
        ]
        residual = [
            residual[j] - step_size * row if j < len(residual) else -(step_size * row)
            for j, row in enumerate(along)
        ]
        if index + 1 < ITERS:
            image = small_map(residual)
            norm_next = reduced([row * row for row in residual])
            product = reduced([row * image[j] for j, row in enumerate(residual)])
            ratio = norm_next / norm_now
            step_size = norm_next / (product - ratio * norm_next / step_size)
            direction = mixed_sum(residual, ratio, direction)
            along = mixed_sum(image, ratio, along)
            norm_now = norm_next
    inverses.append(jnp.ones((1, 1), f32))
    fit_weights = [row[:, 0:1] * inverses[j] for j, row in enumerate(fitted)]
    res_weights = [row[:, 0:1] * inverses[j] for j, row in enumerate(residual)]
    fit = fit_weights[0] * basis[0]
    res = res_weights[0] * basis[0]
    for j in range(1, ITERS):
        fit = fit + fit_weights[j] * basis[j]
        res = res + res_weights[j] * basis[j]
    fit_ref[0] = fit
    res_ref[0] = res + res_weights[ITERS] * basis[ITERS]


def fused_body(factors, heads, tails, values):
    shards = lax.axis_size(("ent", "blk"))
    z_count = lax.axis_size("rel")
    ent_dev, width = factors.shape
    triples = heads.shape[3]
    half = width // 2
    f32, bf16 = jnp.float32, jnp.bfloat16
    vmem = pl.BlockSpec(memory_space=pltpu.VMEM)
    out = pltpu.VMEM((1, width, width), f32)
    share = half // z_count
    return pl.pallas_call(
        functools.partial(
            fused_kernel, z_count, 1.0 / (ent_dev * shards), 1.0 / math.sqrt(shards * triples)
        ),
        out_shape=(out, out),
        in_specs=[pl.BlockSpec(memory_space=pl.ANY)] * 4,
        out_specs=(vmem, vmem),
        scratch_shapes=[
            pltpu.VMEM(factors.shape, bf16),
            pltpu.VMEM(heads.shape, jnp.int32),
            pltpu.VMEM(tails.shape, jnp.int32),
            pltpu.VMEM(values.shape, f32),
            pltpu.SMEM(heads.shape, jnp.int32),
            pltpu.SMEM(tails.shape, jnp.int32),
            pltpu.SemaphoreType.DMA((6,)),
            pltpu.SemaphoreType.REGULAR((max(z_count - 2, 1),)),
            pltpu.VMEM((ent_dev // tile_width, width, tile_width), bf16),
            pltpu.VMEM((width, triples), bf16),
            pltpu.VMEM((width, triples), bf16),
            pltpu.VMEM((width, width), f32),
            pltpu.VMEM((share, width), f32),
            pltpu.VMEM((2, share, width), f32),
            pltpu.VMEM((2, share, width), f32),
            pltpu.VMEM((z_count, share, width), f32),
            pltpu.VMEM((width, width), f32),
            pltpu.VMEM((2, half, width), f32),
            pltpu.VMEM((4, width, width), f32),
            pltpu.VMEM((4, width, width), f32),
            pltpu.VMEM((4, width, width), f32),
            pltpu.VMEM((2, half, width), f32),
            pltpu.VMEM((2, half, width), f32),
            pltpu.VMEM((2, half, width), f32),
            pltpu.VMEM((2, half, width), f32),
            pltpu.VMEM((ITERS + 1, width, width), f32),
            pltpu.VMEM((8, z_count, 1, 128), f32),
            pltpu.SemaphoreType.DMA((COPIES,)),
            pltpu.SemaphoreType.DMA((COPIES,)),
        ],
        compiler_params=pltpu.CompilerParams(collective_id=0, has_side_effects=True),
    )(factors, heads, tails, values)


def solution(mesh):
    placed = (
        P(("ent", "blk"), None),
        P(None, "rel", None, ("ent", "blk")),
        P(None, "rel", None, ("ent", "blk")),
        P(None, "rel", None, ("ent", "blk")),
    )
    sizes = dict(mesh.shape)
    fused = sizes["ent"] == 2 and sizes["blk"] == 4 and sizes["rel"] in (2, 4, 8)
    return jax.shard_map(
        fused_body if fused else body,
        mesh=mesh,
        in_specs=placed,
        out_specs=(P(("ent", "blk", "rel"), None, None), P(("ent", "blk", "rel"), None, None)),
        check_vma=False,
    )
```

```python
import functools
import math

import jax
import jax.numpy as jnp
from jax import lax
from jax.experimental import pallas as pl
from jax.experimental.pallas import tpu as pltpu
from jax.sharding import PartitionSpec as P

ITERS = 8


ridge_weight = 0.01
tile_width = 128


def apply_normal(gram_matrix, stacked):
    left_side = jnp.einsum("ab,kbc->kac", gram_matrix, stacked, precision=lax.Precision.HIGHEST)
    return (
        jnp.einsum("kac,cd->kad", left_side, gram_matrix, precision=lax.Precision.HIGHEST)
        + ridge_weight * stacked
    )


def two_products(residual, image_map):
    return lax.psum(
        (jnp.sum(residual * residual), jnp.sum(residual * image_map)), ("ent", "blk", "rel")
    )


def select_rows(entity_ids, block_table):
    group_size, width = entity_ids.shape
    tile_count = width // tile_width
    block_count = block_table.shape[0]
    tiled_ids = entity_ids.reshape(group_size, tile_count, tile_width)
    block_of = tiled_ids[:, :, 0] // tile_width
    block_pick = (
        block_of[:, :, None] == jnp.arange(block_count, dtype=jnp.int32)[None, None, :]
    ).astype(jnp.bfloat16)
    chosen = jnp.einsum(
        "gtb,bcr->gtcr", block_pick, block_table, preferred_element_type=jnp.float32
    ).astype(jnp.bfloat16)
    inside = tiled_ids % tile_width
    slot_pick = (
        inside[:, :, :, None] == jnp.arange(tile_width, dtype=jnp.int32)[None, None, None, :]
    ).astype(jnp.bfloat16)
    return jnp.einsum("gtoc,gtcr->gtor", slot_pick, chosen, preferred_element_type=jnp.float32)


def body(factors, heads, tails, values):
    shards = lax.axis_size(("ent", "blk"))
    ent_dev = factors.shape[0]
    rank_width = factors.shape[1]
    triple_count = heads.shape[3]
    relation_rows = heads.shape[0] * heads.shape[2]
    norm_scale = 1.0 / math.sqrt(shards * triple_count)
    gram_total = lax.psum(
        jnp.dot(factors.T, factors, preferred_element_type=jnp.float32), ("ent", "blk")
    )
    gram_matrix = gram_total / (ent_dev * shards)
    block_table = factors.reshape(ent_dev // tile_width, tile_width, rank_width)
    head_ids = heads.reshape(relation_rows, triple_count)
    tail_ids = tails.reshape(relation_rows, triple_count)
    weights = values.reshape(relation_rows, triple_count)

    def grouped(operands):
        head_group, tail_group, weight_group = operands
        group_size = head_group.shape[0]
        tile_count = triple_count // tile_width
        head_rows = select_rows(head_group, block_table)
        weighted = (
            weight_group.reshape(group_size, tile_count, tile_width)[:, :, :, None] * head_rows
        ).astype(jnp.bfloat16)
        tail_rows = select_rows(tail_group, block_table).astype(jnp.bfloat16)
        product = jnp.einsum(
            "gtci,gtcj->gij", weighted, tail_rows, preferred_element_type=jnp.float32
        )
        return product * norm_scale

    own_rows = relation_rows // shards
    group_size = math.gcd(own_rows * lax.axis_size(("ent", "blk")), 4)
    group_total = own_rows * lax.axis_size(("ent", "blk")) // group_size
    shaped = (
        head_ids.reshape(group_total, group_size, triple_count),
        tail_ids.reshape(group_total, group_size, triple_count),
        weights.reshape(group_total, group_size, triple_count),
    )
    results = lax.map(grouped, shaped)
    target = lax.psum_scatter(
        results.reshape(own_rows * lax.axis_size(("ent", "blk")), rank_width, rank_width),
        ("ent", "blk"),
        scatter_dimension=0,
        tiled=True,
    )
    fitted = jnp.zeros_like(target)
    residual = target
    image_map = apply_normal(gram_matrix, residual)
    norm_now, product = two_products(residual, image_map)
    step_size = norm_now / product
    direction = residual
    along = image_map
    for step_index in range(ITERS):
        fitted = fitted + step_size * direction
        residual = residual - step_size * along
        if step_index + 1 < ITERS:
            image_map = apply_normal(gram_matrix, residual)
            norm_next, product = two_products(residual, image_map)
            ratio_next = norm_next / norm_now
            step_size = norm_next / (product - ratio_next * norm_next / step_size)
            direction = residual + ratio_next * direction
            along = image_map + ratio_next * along
            norm_now = norm_next
    return (fitted, residual)


MESH = pl.DeviceIdType.MESH
COPIES = 64


def fused_kernel(
    z_count, scale_gram, scale_target,
    factors_hbm, heads_hbm, tails_hbm, values_hbm,
    fit_ref, res_ref,
    factors_ref, heads_ref, tails_ref, values_ref, head_ids, tail_ids, load_sem, ready,
    turned, left_rows, right_rows,
    gram_part, gram_in, gram_half, gram_xy, gram_line, gram_full, gram_pair,
    pair_out, pair_in, own_sum, first_a, first_b, second_a, second_b,
    basis, table, send_sem, recv_sem,
):
    f32, bf16 = jnp.float32, jnp.bfloat16
    width = factors_ref.shape[1]
    half = width // 2
    share = half // z_count
    part = share // 2
    triples = heads_ref.shape[3]
    e = lax.axis_index("ent")
    b = lax.axis_index("blk")
    z = lax.axis_index("rel")
    y = b // 2
    c = b % 2
    pair_peer = (e, y * 2 + 1 - c, z)
    x_peer = (1 - e, b, z)
    y_peer = (e, (1 - y) * 2 + c, z)

    def group_peer(mask):
        me, my, mc = mask // 4, (mask // 2) % 2, mask % 2
        return (
            (1 - e) if me else e,
            ((1 - y) if my else y) * 2 + ((1 - c) if mc else c),
            z,
        )

    def z_peer(hop):
        return (e, b, lax.rem(z + hop, z_count))

    near = [group_peer(m) for m in (1, 2, 4)]
    inner = ((z > 0, -1), (z < z_count - 1, 1))

    def tell(semaphore):
        for present, hop in inner:
            @pl.when(present)
            def _():
                pl.semaphore_signal(
                    semaphore, inc=1, device_id=(e, b, z + hop), device_id_type=MESH
                )

    line_count = jnp.where(z > 0, 1, 0) + jnp.where(z < z_count - 1, 1, 0)
    barrier = pltpu.get_barrier_semaphore()
    for peer in near:
        pl.semaphore_signal(barrier, inc=1, device_id=peer, device_id_type=MESH)
    tell(barrier)
    loads = []
    for slot, (source, dest) in enumerate(
        (
            (factors_hbm, factors_ref),
            (heads_hbm, head_ids),
            (tails_hbm, tail_ids),
            (heads_hbm, heads_ref),
            (values_hbm, values_ref),
            (tails_hbm, tails_ref),
        )
    ):
        loads.append(pltpu.make_async_copy(source, dest, load_sem.at[slot]))
        loads[-1].start()

    counter = [0]

    def send(source, dest, peer):
        slot = counter[0]
        counter[0] += 1
        copy = pltpu.make_async_remote_copy(
            src_ref=source, dst_ref=dest,
            send_sem=send_sem.at[slot], recv_sem=recv_sem.at[slot],
            device_id=peer, device_id_type=MESH,
        )
        copy.start()
        return copy

    loads[0].wait()
    flipped = factors_ref[...].T
    for block in range(turned.shape[0]):
        turned[block] = flipped[:, block * tile_width : (block + 1) * tile_width]
    gram_part[...] = lax.dot_general(
        flipped, flipped, (((1,), (1,)), ((), ())), preferred_element_type=f32
    )
    own_rows = pl.ds(pl.multiple_of(c * half, half), half)
    other_rows = pl.ds(pl.multiple_of((1 - c) * half, half), half)
    own_share = pl.ds(pl.multiple_of(c * half + z * share, share), share)
    other_share = pl.ds(pl.multiple_of((1 - c) * half + z * share, share), share)

    row_number = lax.broadcasted_iota(jnp.int32, (tile_width, tile_width), 0)
    blank = jnp.zeros((tile_width, tile_width), bf16)

    def gathered(ids_ref, scalar_ref, q, first):
        picks, blocks = [], []
        for tile in (first, first + 1):
            start = tile * tile_width
            inside = lax.rem(ids_ref[q, 0, :, start : start + tile_width], tile_width)
            picks.append(jnp.where(row_number == inside, 1.0, 0.0).astype(bf16))
            blocks.append(turned[lax.div(scalar_ref[q, 0, 0, start], tile_width)])
        mixed = jnp.concatenate(
            [
                jnp.concatenate([picks[0], blank], axis=1),
                jnp.concatenate([blank, picks[1]], axis=1),
            ],
            axis=0,
        )
        return jnp.dot(jnp.concatenate(blocks, axis=1), mixed, preferred_element_type=f32)

    def partial(pe, py, pc):
        q = pe * 4 + py * 2 + pc
        for first in range(0, triples // tile_width, 2):
            cols = slice(first * tile_width, (first + 2) * tile_width)
            rows = gathered(heads_ref, head_ids, q, first)
            left_rows[:, cols] = (values_ref[q, 0, :, cols] * rows).astype(bf16)
            right_rows[:, cols] = gathered(tails_ref, tail_ids, q, first).astype(bf16)
        return lax.dot_general(
            left_rows[...], right_rows[...], (((1,), (1,)), ((), ())), preferred_element_type=f32
        )

    targets = ((1 - e, 1 - y), (1 - e, y), (e, 1 - y), (e, y))
    pair_copies = []

    def give(index):
        pe, py = targets[index]
        pair_out[index] = partial(pe, py, 1 - c)
        pair_copies.append(send(pair_out.at[index], pair_in.at[index], pair_peer))

    def keep(index):
        pe, py = targets[index]
        own_sum[index] = partial(pe, py, c)
        pair_copies[index].wait()
        own_sum[index] = own_sum[index] + pair_in[index]

    top, low = pl.ds(0, half), pl.ds(half, half)
    for load in loads[1:]:
        load.wait()
    pair_out[0] = partial(1 - e, 1 - y, 1 - c)
    pl.semaphore_wait(barrier, len(near) + line_count)
    g_pair = send(gram_part.at[other_share], gram_in, pair_peer)
    pair_copies.append(send(pair_out.at[0], pair_in.at[0], pair_peer))
    for step in range(z_count - 2):
        tell(ready.at[step])
        if step + 1 < z_count - 2:
            pl.semaphore_wait(ready.at[step], line_count)
    g_pair.wait()
    gram_half[0] = gram_part[own_share, :] + gram_in[...]
    upper, lower = pl.ds(0, part), pl.ds(part, part)
    g_a1 = send(gram_half.at[0, upper], gram_xy.at[0, upper], x_peer)
    g_b1 = send(gram_half.at[0, lower], gram_xy.at[0, lower], y_peer)
    keep(0)
    a_diag = send(own_sum.at[0, top], first_a.at[0], x_peer)
    b_diag = send(own_sum.at[0, low], first_b.at[0], y_peer)
    give(1)
    g_a1.wait()
    g_b1.wait()
    gram_half[1] = gram_half[0] + gram_xy[0]
    g_a2 = send(gram_half.at[1, upper], gram_xy.at[1, upper], y_peer)
    g_b2 = send(gram_half.at[1, lower], gram_xy.at[1, lower], x_peer)
    keep(1)
    a_side = send(own_sum.at[1, top], first_a.at[1], x_peer)
    give(2)
    g_a2.wait()
    g_b2.wait()
    gram_line[0] = gram_half[1] + gram_xy[1]
    if z_count > 2:
        pl.semaphore_wait(ready.at[z_count - 3], line_count)
    line_copies = [
        send(gram_line.at[0], gram_line.at[z_count - hop], z_peer(hop))
        for hop in range(1, z_count)
    ]
    keep(2)
    b_side = send(own_sum.at[2, low], first_b.at[1], y_peer)
    a_diag.wait()
    second_a[0] = own_sum[2, :half, :] + first_a[0]
    a_last = send(second_a.at[0], second_a.at[1], y_peer)
    b_diag.wait()
    second_b[0] = own_sum[1, half:, :] + first_b[0]
    b_last = send(second_b.at[0], second_b.at[1], x_peer)
    give(3)
    keep(3)
    for copy in line_copies:
        copy.wait()
    for hop in range(z_count):
        place = lax.rem(z + hop, z_count)
        gram_pair[0, pl.ds(pl.multiple_of(place * share, share), share), :] = gram_line[hop]
    g_full = send(gram_pair.at[0], gram_pair.at[1], pair_peer)
    g_full.wait()
    gram_full[own_rows, :] = gram_pair[0] * scale_gram
    gram_full[other_rows, :] = gram_pair[1] * scale_gram
    gram = gram_full[...]
    gram_high = gram.astype(bf16)
    gram_low = (gram - gram_high.astype(f32)).astype(bf16)
    gram_both = jnp.concatenate([gram_high, gram_low], axis=0)
    a_side.wait()
    b_side.wait()
    a_last.wait()
    b_last.wait()
    basis[0, :half, :] = ((own_sum[3, :half, :] + first_a[1]) + second_a[1]) * scale_target
    basis[0, half:, :] = ((own_sum[3, half:, :] + first_b[1]) + second_b[1]) * scale_target

    def split(value):
        high = value.astype(bf16)
        return high, (value - high.astype(f32)).astype(bf16)

    def total(value):
        return jnp.sum(jnp.sum(value, axis=0, keepdims=True), axis=1, keepdims=True)

    def normal_map(value):
        high, low_part = split(value)
        both = jnp.dot(gram_both, high, preferred_element_type=f32)
        inner = both[:width] + (
            both[width:] + jnp.dot(gram_high, low_part, preferred_element_type=f32)
        )
        high, low_part = split(inner)
        both = jnp.dot(
            jnp.concatenate([high, low_part], axis=0), gram_high, preferred_element_type=f32
        )
        outer = both[:width] + (
            both[width:] + jnp.dot(high, gram_low, preferred_element_type=f32)
        )
        return outer + ridge_weight * value

    lane = lax.broadcasted_iota(jnp.int32, (1, 128), 1)
    record = jnp.zeros((1, 128), f32)
    inverses = []
    for index in range(ITERS):
        vector = basis[index]
        image = normal_map(vector)
        square = total(vector * vector)
        cross = total(vector * image)
        inverse = jnp.where(square > 0.0, lax.rsqrt(square), 0.0)
        length = square * inverse
        diagonal = (cross * inverse) * inverse
        record = jnp.where(lane == index, diagonal, record)
        record = jnp.where(lane == ITERS + index, length, record)
        if index + 1 == ITERS:
            table[0, 0] = record
            far_copies = [
                send(
                    table.at[0, 0],
                    table.at[m, (z_count - hop) % z_count],
                    group_peer(m)[:2] + (lax.rem(z + hop, z_count),),
                )
                for hop in range(z_count)
                for m in range(8)
                if m or hop
            ]
        following = (image - diagonal * vector) * inverse
        if index > 0:
            following = following - (length * inverses[-1]) * basis[index - 1]
        inverses.append(inverse)
        basis[index + 1] = following
    for copy in far_copies:
        copy.wait()

    lines = table[...].reshape(8 * z_count, 128)
    filled = jnp.concatenate([lines, jnp.zeros((128 - 8 * z_count, 128), f32)], axis=0).T
    alpha = [filled[j : j + 1, :] for j in range(ITERS)]
    beta = [filled[ITERS + j : ITERS + j + 1, :] for j in range(ITERS)] + [
        jnp.ones((1, 128), f32)
    ]

    def reduced(rows):
        added = rows[0]
        for row in rows[1:]:
            added = added + row
        return jnp.sum(added, axis=1, keepdims=True)

    def small_map(rows):
        count = len(rows)
        made = []
        for j in range(count + 1):
            entry = None
            if j < count:
                entry = alpha[j] * rows[j]
            if j > 0:
                term = beta[j] * rows[j - 1]
                entry = term if entry is None else entry + term
            if j + 1 < count:
                entry = entry + beta[j + 1] * rows[j + 1]
            made.append(entry)
        return made

    def mixed_sum(first, ratio, second):
        return [
            one + ratio * second[j] if j < len(second) else one for j, one in enumerate(first)
        ]

    residual = [beta[0]]
    image = small_map(residual)
    norm_now = reduced([row * row for row in residual])
    product = reduced([row * image[j] for j, row in enumerate(residual)])
    step_size = norm_now / product
    direction, along = residual, image
    fitted = []
    for index in range(ITERS):
        fitted = [
            fitted[j] + step_size * row if j < len(fitted) else step_size * row
            for j, row in enumerate(direction)
        ]
        residual = [
            residual[j] - step_size * row if j < len(residual) else -(step_size * row)
            for j, row in enumerate(along)
        ]
        if index + 1 < ITERS:
            image = small_map(residual)
            norm_next = reduced([row * row for row in residual])
            product = reduced([row * image[j] for j, row in enumerate(residual)])
            ratio = norm_next / norm_now
            step_size = norm_next / (product - ratio * norm_next / step_size)
            direction = mixed_sum(residual, ratio, direction)
            along = mixed_sum(image, ratio, along)
            norm_now = norm_next
    inverses.append(jnp.ones((1, 1), f32))
    fit_weights = [row[:, 0:1] * inverses[j] for j, row in enumerate(fitted)]
    res_weights = [row[:, 0:1] * inverses[j] for j, row in enumerate(residual)]
    fit = fit_weights[0] * basis[0]
    res = res_weights[0] * basis[0]
    for j in range(1, ITERS):
        fit = fit + fit_weights[j] * basis[j]
        res = res + res_weights[j] * basis[j]
    fit_ref[0] = fit
    res_ref[0] = res + res_weights[ITERS] * basis[ITERS]


def fused_body(factors, heads, tails, values):
    shards = lax.axis_size(("ent", "blk"))
    z_count = lax.axis_size("rel")
    ent_dev, width = factors.shape
    triples = heads.shape[3]
    half = width // 2
    f32, bf16 = jnp.float32, jnp.bfloat16
    vmem = pl.BlockSpec(memory_space=pltpu.VMEM)
    out = pltpu.VMEM((1, width, width), f32)
    share = half // z_count
    return pl.pallas_call(
        functools.partial(
            fused_kernel, z_count, 1.0 / (ent_dev * shards), 1.0 / math.sqrt(shards * triples)
        ),
        out_shape=(out, out),
        in_specs=[pl.BlockSpec(memory_space=pl.ANY)] * 4,
        out_specs=(vmem, vmem),
        scratch_shapes=[
            pltpu.VMEM(factors.shape, bf16),
            pltpu.VMEM(heads.shape, jnp.int32),
            pltpu.VMEM(tails.shape, jnp.int32),
            pltpu.VMEM(values.shape, f32),
            pltpu.SMEM(heads.shape, jnp.int32),
            pltpu.SMEM(tails.shape, jnp.int32),
            pltpu.SemaphoreType.DMA((6,)),
            pltpu.SemaphoreType.REGULAR((max(z_count - 2, 1),)),
            pltpu.VMEM((ent_dev // tile_width, width, tile_width), bf16),
            pltpu.VMEM((width, triples), bf16),
            pltpu.VMEM((width, triples), bf16),
            pltpu.VMEM((width, width), f32),
            pltpu.VMEM((share, width), f32),
            pltpu.VMEM((2, share, width), f32),
            pltpu.VMEM((2, share, width), f32),
            pltpu.VMEM((z_count, share, width), f32),
            pltpu.VMEM((width, width), f32),
            pltpu.VMEM((2, half, width), f32),
            pltpu.VMEM((4, width, width), f32),
            pltpu.VMEM((4, width, width), f32),
            pltpu.VMEM((4, width, width), f32),
            pltpu.VMEM((2, half, width), f32),
            pltpu.VMEM((2, half, width), f32),
            pltpu.VMEM((2, half, width), f32),
            pltpu.VMEM((2, half, width), f32),
            pltpu.VMEM((ITERS + 1, width, width), f32),
            pltpu.VMEM((8, z_count, 1, 128), f32),
            pltpu.SemaphoreType.DMA((COPIES,)),
            pltpu.SemaphoreType.DMA((COPIES,)),
        ],
        compiler_params=pltpu.CompilerParams(collective_id=0, has_side_effects=True),
    )(factors, heads, tails, values)


def solution(mesh):
    placed = (
        P(("ent", "blk"), None),
        P(None, "rel", None, ("ent", "blk")),
        P(None, "rel", None, ("ent", "blk")),
        P(None, "rel", None, ("ent", "blk")),
    )
    sizes = dict(mesh.shape)
    fused = sizes["ent"] == 2 and sizes["blk"] == 4 and sizes["rel"] in (2, 4, 8)
    return jax.shard_map(
        fused_body if fused else body,
        mesh=mesh,
        in_specs=placed,
        out_specs=(P(("ent", "blk", "rel"), None, None), P(("ent", "blk", "rel"), None, None)),
        check_vma=False,
    )
```
